512 devices in a mesh: dp: 8 (over y_hi, core), ep: 64 (over x, y_lo, z).
Axes of the slice: x: 4, y: 8 (y_hi: 4, y_lo: 2; y = y_hi * 2 + y_lo), z: 8, core: 2. Of those that a mesh axis runs over, the one named last changes fastest.
Arguments:
- hidden_in: bfloat16 [12288, 4096], P(('dp', 'ep')), may hold values from -6 to 6
- expert_ids: int32 [12288, 2], P(('dp', 'ep')), may hold values from 0 to 63, all different within a row; in each aligned block of 24 rows (0 to 23, 24 to 47, ...) at most 2 rows name the same one
- route_logits: float32 [12288, 64], P(('dp', 'ep')), may hold values from -10 to 10
- first_weight: bfloat16 [64, 4096, 1024], P('ep', None, 'dp'), may hold values from -0.09375 to 0.09375
- second_weight: bfloat16 [64, 1024, 4096], P('ep', None, 'dp'), may hold values from -0.1875 to 0.1875
- queries: bfloat16 [12288, 2048], P(('dp', 'ep')), may hold values from -140 to 140
- span_keys: bfloat16 [12288, 2048], P(('dp', 'ep')), may hold values from -7 to 7
- span_values: bfloat16 [12288, 2048], P(('dp', 'ep')), may hold values from -6 to 6
- cache_keys: bfloat16 [512, 72, 2048], P(('dp', 'ep')), may hold values from -6 to 6
- cache_values: bfloat16 [512, 72, 2048], P(('dp', 'ep')), may hold values from -6 to 6
- valid_frames: int32 [512], P(('dp', 'ep')), may hold values from 1 to 3
Outputs:
- mixed: bfloat16 [12288, 4096], P(('dp', 'ep'))
- attended: bfloat16 [12288, 2048], P(('dp', 'ep'))
The draws below stay inside these ranges and needn't reach their ends.
Inputs may be any that keep to these rules, and one draw needn't show every extreme that they name: `expert_ids`: each token names two different experts. In the rows of one device (24 rows) no expert is named more than 2 times, a bound that some block reaches.
All inputs are finite; a program needn't handle non-finite values.
Results may differ from the reference program's by a relative error of at most 0.0057.
Values may be sent and summed in bfloat16 or wider, within the bound.
No kernel may reach another device: no remote copies, remote signals or barrier semaphores. Data moves between devices by JAX's collectives and lax.ppermute only.
A program may use at most 128 MiB of HBM per device.

```python
import math
import jax
import jax.numpy as jnp
import numpy as np
from jax import lax

D = 4096
FFN = 1024
HEADS = 16
HEAD_DIM = 128
TOK = 24
FRAME_TOK = 24
CFRAMES = 3
CACHE_TOK = 72
EXPERTS = 64
STREAMS = 512
TOKENS = 12288
CAP = 2


def query_key_pair(key):
    width = HEADS * HEAD_DIM
    key_rows = jnp.clip(jax.random.normal(jax.random.fold_in(key, 101), (TOKENS, width), jnp.float32), -6.0, 6.0)
    query_rows = jnp.clip(jax.random.normal(jax.random.fold_in(key, 202), (TOKENS, width), jnp.float32), -6.0, 6.0)
    return (query_rows, key_rows)


def draw_queries(key, part):
    query_rows, key_rows = query_key_pair(key)
    return query_rows.astype(jnp.bfloat16)


def draw_span_keys(key, part):
    query_rows, key_rows = query_key_pair(key)
    return key_rows.astype(jnp.bfloat16)


def set_ends(entries, own_key, low, largest):
    longest = entries.shape.index(max(entries.shape))
    spots = []
    for shift in (0, 1):
        where = [jax.random.randint(jax.random.fold_in(own_key, axis), (), 0, length) for axis, length in enumerate(entries.shape)]
        where[longest] = (where[longest] + shift) % entries.shape[longest]
        spots.append(tuple(where))
    return entries.at[spots[0]].set(low).at[spots[1]].set(largest)


def steps_of(stream_key, dims, pieces, low, high):
    loudness, own = 1.0, jax.random.fold_in(stream_key, 6)
    for dim, shards_of in pieces:
        steps = jnp.exp(jax.random.uniform(jax.random.fold_in(own, dim), (shards_of,), jnp.float32, low / len(pieces), high / len(pieces)))
        loudness = loudness * jnp.repeat(steps, dims[dim] // shards_of).reshape([-1 if axis == dim else 1 for axis in range(len(dims))])
    return loudness


def assign_block(stream_key, own, number, rows, count, top, reach, lean):
    ranking = jax.random.permutation(stream_key, count)
    crowded, ordinary = load_shares(count, rows * top, reach, lean, True), load_shares(count, rows * top, reach, lean, False)
    places = jnp.arange(count)

    def named(lengths, offset_by):
        used = int((lengths > 0).sum())
        fixed = max(1, used // 4)
        passed = fixed + (places - fixed + offset_by * (used - fixed)) % max(1, count - fixed)
        return jnp.zeros((count,), jnp.int32).at[ranking[jnp.where(places < fixed, places, passed)]].set(jnp.asarray(lengths, jnp.int32))

    lengths = jnp.where(number % 4 == 0, named(crowded, number // 4), named(ordinary, number - number // 4 - 1))
    mixed = jax.random.permutation(jax.random.fold_in(own, 3), count)
    giver, receiver = mixed[0:count // 2 * 2:2], mixed[1:count // 2 * 2:2]
    margin = jnp.minimum(lengths[giver] - 1, reach - lengths[receiver]) // 2
    margin = jnp.where((giver == ranking[0]) | (receiver == ranking[0]) | (lengths[receiver] == 0), 0, jnp.maximum(margin, 0))
    passed = jax.random.randint(jax.random.fold_in(own, 4), (count // 2,), 0, 1 << 20) % (margin + 1)
    lengths = lengths.at[giver].add(-passed).at[receiver].add(passed)
    members = jnp.searchsorted(jnp.cumsum(lengths), jnp.arange(rows * top), side="right").astype(jnp.int32)
    listing = members.reshape(top, rows).T
    listing = listing[jax.random.permutation(jax.random.fold_in(own, 1), rows)]
    offset_by = jax.random.randint(jax.random.fold_in(own, 2), (rows, 1), 0, top)
    return jnp.take_along_axis(listing, (jnp.arange(top)[None, :] + offset_by) % top, axis=1)


def load_shares(amount, total, bound, lean, full):
    portions = [(1 << 20) // math.isqrt(rank ** lean) + 1 for rank in range(1, amount + 1)]
    largest = bound if full else min(bound, max(-(-total // amount), total * portions[0] // sum(portions)))
    least = 1 if total - largest >= amount - 1 else 0
    given, surplus = [largest] + [least] * (amount - 1), total - largest - least * (amount - 1)
    while surplus > 0:
        candidates = [i for i in range(1, amount) if given[i] < largest] or [i for i in range(1, amount) if given[i] < bound]
        pool, left = sum([portions[i] for i in candidates]), surplus
        for i in candidates:
            extra = min(bound - given[i], max(1, left * portions[i] // pool), surplus)
            given[i] = given[i] + extra
            surplus = surplus - extra
    return np.array(given)


def centred(key, extent, deviation, limit, pieces=(), kind=jnp.bfloat16):
    array = deviation * jax.random.normal(key, extent, jnp.float32)
    if pieces:
        array = array * steps_of(key, extent, pieces, -0.22, 0.18)
    return jnp.clip(array, -limit, limit).astype(kind)


def setup_inputs(seed: int = 0) -> dict:
    key_list = jax.random.split(jax.random.key(seed), 12)
    hidden_in = centred(key_list[0], (TOKENS, D), 1.0, 6.0, ((0, 512),))
    expert_ids_keys = jax.random.split(jax.random.fold_in(key_list[1], 1), TOKENS // TOK)
    expert_ids_turns = jax.random.permutation(jax.random.fold_in(key_list[1], 3), TOKENS // TOK)
    expert_ids = jax.vmap(lambda own, number: assign_block(jax.random.fold_in(key_list[1], 2), own, number, TOK, EXPERTS, 2, CAP, 2))(expert_ids_keys, expert_ids_turns).reshape((TOKENS, 2))
    route_logits = centred(key_list[2], (TOKENS, EXPERTS), 2.0, 10.0, ((0, 512),), jnp.float32)
    first_weight = centred(key_list[3], (EXPERTS, D, FFN), D ** -0.5, 0.09375, ((0, 64), (2, 8)))
    second_weight = centred(key_list[4], (EXPERTS, FFN, D), FFN ** -0.5, 0.1875, ((0, 64), (2, 8)))
    queries = draw_queries(jax.random.fold_in(key_list[11], 71), 0)
    span_keys = draw_span_keys(jax.random.fold_in(key_list[11], 71), 0)
    span_values = centred(key_list[7], (TOKENS, HEADS * HEAD_DIM), 1.0, 6.0, ((0, 512),))
    cache_keys = centred(key_list[8], (STREAMS, CACHE_TOK, HEADS * HEAD_DIM), 1.0, 6.0, ((0, 512),))
    cache_values = centred(key_list[9], (STREAMS, CACHE_TOK, HEADS * HEAD_DIM), 1.0, 6.0, ((0, 512),))
    valid_frames = set_ends(jax.random.randint(key_list[10], (STREAMS,), 1, CFRAMES + 1), jax.random.fold_in(key_list[10], 1), 1, CFRAMES).astype(jnp.int32)
    return dict(hidden_in=hidden_in, expert_ids=expert_ids, route_logits=route_logits, first_weight=first_weight, second_weight=second_weight, queries=queries, span_keys=span_keys, span_values=span_values, cache_keys=cache_keys, cache_values=cache_values, valid_frames=valid_frames)


def activate(pre):
    return jax.nn.gelu(pre, approximate=True).astype(jnp.bfloat16)

def attend(queries, span_keys, span_values, cache_keys, cache_values, valid_count):
    token_count = queries.shape[0]
    cache_len = cache_keys.shape[0]
    key_rows = jnp.concatenate([cache_keys, span_keys], axis=0)
    value_rows = jnp.concatenate([cache_values, span_values], axis=0)
    query_heads = queries.reshape(token_count, HEADS, HEAD_DIM).astype(jnp.float32)
    key_heads = key_rows.reshape(-1, HEADS, HEAD_DIM).astype(jnp.float32)
    value_heads = value_rows.reshape(-1, HEADS, HEAD_DIM).astype(jnp.float32)
    scores = jnp.einsum('thd,khd->htk', query_heads, key_heads) * (1.0 / math.sqrt(HEAD_DIM))
    position = jnp.arange(key_rows.shape[0], dtype=jnp.int32)
    usable = (position >= cache_len) | (position // FRAME_TOK < valid_count)
    scores = jnp.where(usable[None, None, :], scores, -1e+30)
    row_max = lax.optimization_barrier(jnp.max(scores, axis=2, keepdims=True))
    weights = jnp.exp(scores - row_max)
    weights = (weights / lax.optimization_barrier(jnp.sum(weights, axis=2, keepdims=True))).astype(jnp.bfloat16)
    result = jnp.einsum('htk,khd->thd', weights.astype(jnp.float32), value_heads)
    return result.astype(jnp.bfloat16).reshape(token_count, HEADS * HEAD_DIM)

def block_slots(expert_ids):
    assigned = TOK * 2
    blocks = expert_ids.reshape(STREAMS, assigned)
    row_ids = lax.broadcasted_iota(jnp.int32, (assigned, assigned), 0)
    col_ids = lax.broadcasted_iota(jnp.int32, (assigned, assigned), 1)

    def per_block(flat_ids):
        same_expert = (flat_ids[:, None] == flat_ids[None, :]) & (col_ids < row_ids)
        return lax.optimization_barrier(jnp.sum(same_expert.astype(jnp.int32), axis=1))
    return jax.vmap(per_block)(blocks).reshape(TOKENS, 2)

def reference(hidden_in, expert_ids, route_logits, first_weight, second_weight, queries, span_keys, span_values, cache_keys, cache_values, valid_frames):
    slots = block_slots(expert_ids)
    token_index = jnp.arange(TOKENS, dtype=jnp.int32)
    stream_of = token_index // TOK
    rows_at = (stream_of[:, None] * CAP + slots).astype(jnp.int32)
    slot_table = jnp.full((EXPERTS, STREAMS * CAP), TOKENS, jnp.int32)
    slot_table = slot_table.at[expert_ids, rows_at].set(jnp.broadcast_to(token_index[:, None], (TOKENS, 2)))
    padded = jnp.concatenate([hidden_in, jnp.zeros((1, D), jnp.bfloat16)], axis=0)

    def apply_expert(operands):
        first_matrix, second_matrix, index_row = operands
        expert_rows = padded[index_row]
        hidden = activate(jnp.dot(expert_rows, first_matrix, preferred_element_type=jnp.float32))
        return jnp.dot(hidden, second_matrix, preferred_element_type=jnp.float32).astype(jnp.bfloat16)
    expert_outs = lax.map(apply_expert, (first_weight, second_weight, slot_table))
    chosen = jnp.take_along_axis(route_logits, expert_ids, axis=1)
    gates = jax.nn.softmax(chosen, axis=1)
    running = jnp.zeros((TOKENS, D), jnp.float32)
    for column in range(2):
        picked = expert_outs[expert_ids[:, column], rows_at[:, column]].astype(jnp.float32)
        running = running + gates[:, column:column + 1] * picked
    mixed = running.astype(jnp.bfloat16)
    width = HEADS * HEAD_DIM
    attended = jax.vmap(attend)(queries.reshape(STREAMS, TOK, width), span_keys.reshape(STREAMS, TOK, width), span_values.reshape(STREAMS, TOK, width), cache_keys, cache_values, valid_frames).reshape(TOKENS, width)
    return (mixed, attended)
```

```python
import math

import jax
import jax.numpy as jnp
from jax import lax
from jax.sharding import PartitionSpec as P

HEADS = 16
HEAD_DIM = 128
FRAME_TOK = 24

WEIGHT_MATE = (1, 0, 3, 2)
ROW_MATE = (3, 2, 1, 0)


def ring_swap(mate):
    return [(2 * ring + core, 2 * mate[ring] + core) for ring in range(4) for core in range(2)]


WEIGHT_SWAP = ring_swap(WEIGHT_MATE)
ROW_SWAP = ring_swap(ROW_MATE)
CORE_SWAP = [(place, place ^ 1) for place in range(8)]


def activate(pre):
    return jax.nn.gelu(pre, approximate=True).astype(jnp.bfloat16)


def expert_slots(expert_ids):
    flat_ids = expert_ids.reshape(-1)
    assigned = flat_ids.shape[0]
    row_ids = lax.broadcasted_iota(jnp.int32, (assigned, assigned), 0)
    col_ids = lax.broadcasted_iota(jnp.int32, (assigned, assigned), 1)
    same_expert = (flat_ids[:, None] == flat_ids[None, :]) & (col_ids < row_ids)
    return jnp.sum(same_expert.astype(jnp.int32), axis=1).reshape(expert_ids.shape)


def attend(queries, span_keys, span_values, cache_keys, cache_values, valid_count):
    token_count = queries.shape[0]
    cache_len = cache_keys.shape[0]
    key_rows = jnp.concatenate([cache_keys, span_keys], axis=0)
    value_rows = jnp.concatenate([cache_values, span_values], axis=0)
    query_heads = queries.reshape(token_count, HEADS, HEAD_DIM)
    key_heads = key_rows.reshape(-1, HEADS, HEAD_DIM)
    value_heads = value_rows.reshape(-1, HEADS, HEAD_DIM)
    scores = jnp.einsum(
        "thd,khd->htk", query_heads, key_heads, preferred_element_type=jnp.float32
    ) * (1.0 / math.sqrt(HEAD_DIM))
    position = lax.broadcasted_iota(jnp.int32, (key_rows.shape[0],), 0)
    usable = (position >= cache_len) | (position // FRAME_TOK < valid_count)
    scores = jnp.where(usable[None, None, :], scores, -1e30)
    row_max = jnp.max(scores, axis=2, keepdims=True)
    weights = jnp.exp(scores - row_max)
    weights = (weights / jnp.sum(weights, axis=2, keepdims=True)).astype(jnp.bfloat16)
    result = jnp.einsum("htk,khd->thd", weights, value_heads, preferred_element_type=jnp.float32)
    return result.astype(jnp.bfloat16).reshape(token_count, HEADS * HEAD_DIM)


def in_order(swapped, first, second):
    return [jnp.where(swapped, second, first), jnp.where(swapped, first, second)]


def pair_order(ring, core, blocks):
    own = jnp.concatenate(in_order(core == 1, blocks[0], blocks[1]), axis=1)
    mate = jnp.concatenate(in_order(core == 1, blocks[2], blocks[3]), axis=1)
    return jnp.concatenate(in_order(ring % 2 == 1, own, mate), axis=1)


def both_cores(block):
    mate = lax.ppermute(block, "dp", WEIGHT_SWAP)
    return [
        block,
        lax.ppermute(block, "dp", CORE_SWAP),
        mate,
        lax.ppermute(mate, "dp", CORE_SWAP),
    ]


def shards(
    hidden_in,
    expert_ids,
    route_logits,
    first_weight,
    second_weight,
    queries,
    span_keys,
    span_values,
    cache_keys,
    cache_values,
    valid_frames,
):
    tokens, model_width = hidden_in.shape
    experts = lax.axis_size("ep")
    place = lax.axis_index("dp")
    ring, core = place // 2, place % 2
    upper = ring // 2

    with jax.named_scope("weights"):
        first_parts = both_cores(first_weight[0])
        second_parts = both_cores(second_weight[0])

    with jax.named_scope("route"):
        slots = expert_slots(expert_ids)
        places = expert_ids * 4 + upper * 2 + slots
        expert_cols = lax.broadcasted_iota(jnp.int32, route_logits.shape, 1)
        chosen = jnp.stack(
            [
                jnp.sum(
                    jnp.where(expert_cols == expert_ids[:, column : column + 1], route_logits, 0.0),
                    axis=1,
                )
                for column in range(2)
            ],
            axis=1,
        )
        gates = jax.nn.softmax(chosen, axis=1)
        notes = jnp.concatenate([places.astype(jnp.float32), gates], axis=1)
        both_notes = jnp.concatenate([notes, lax.ppermute(notes, "dp", ROW_SWAP)], axis=0)
        both_places = both_notes[:, :2].astype(jnp.int32)
        both_gates = both_notes[:, 2:]
        both_hidden = jnp.concatenate(
            [hidden_in, lax.ppermute(hidden_in, "dp", ROW_SWAP)], axis=0
        )
        place_ids = lax.broadcasted_iota(jnp.int32, (2 * tokens, experts * 4), 1)
        picks = [both_places[:, column : column + 1] == place_ids for column in range(2)]
        chooser = (picks[0] | picks[1]).astype(jnp.bfloat16)

    with jax.named_scope("dispatch"):
        dispatch = lax.dot_general(
            chooser, both_hidden, (((0,), (0,)), ((), ())), preferred_element_type=jnp.float32
        )
        dispatch = dispatch.astype(jnp.bfloat16).reshape(experts, 4, model_width)
        received = lax.all_to_all(dispatch, "ep", split_axis=0, concat_axis=0, tiled=True)
        expert_rows = received.reshape(experts * 4, model_width)

    with jax.named_scope("first"):
        act = pair_order(
            ring,
            core,
            [
                activate(jnp.dot(expert_rows, part, preferred_element_type=jnp.float32))
                for part in first_parts
            ],
        )
        other_act = lax.ppermute(act, "dp", ROW_SWAP)
        all_act = jnp.concatenate(in_order(upper == 1, act, other_act), axis=1)

    with jax.named_scope("second"):
        outputs = jnp.concatenate(
            [
                jnp.dot(all_act, part, preferred_element_type=jnp.float32).astype(jnp.bfloat16)
                for part in second_parts
            ],
            axis=1,
        )
        returned = lax.all_to_all(
            outputs.reshape(experts, 4, -1), "ep", split_axis=0, concat_axis=0, tiled=True
        )
        flat_back = returned.reshape(experts * 4, -1)

    with jax.named_scope("attention"):
        attended = attend(
            queries, span_keys, span_values, cache_keys[0], cache_values[0], valid_frames[0]
        )

    with jax.named_scope("combine"):
        running = jnp.zeros((2 * tokens, flat_back.shape[1]), jnp.float32)
        for column in range(2):
            picked = jnp.dot(
                picks[column].astype(jnp.bfloat16), flat_back, preferred_element_type=jnp.float32
            )
            running = running + both_gates[:, column : column + 1] * picked
        mixed = running.astype(jnp.bfloat16)
        mixed = pair_order(ring, core, jnp.split(mixed, 4, axis=1))
        other_mixed = lax.ppermute(mixed[tokens:], "dp", ROW_SWAP)
        mixed = jnp.concatenate(in_order(upper == 1, mixed[:tokens], other_mixed), axis=1)
    return (mixed, attended)


def solution(mesh):
    placed = (
        P(("dp", "ep"), None),
        P(("dp", "ep"), None),
        P(("dp", "ep"), None),
        P("ep", None, "dp"),
        P("ep", None, "dp"),
        P(("dp", "ep"), None),
        P(("dp", "ep"), None),
        P(("dp", "ep"), None),
        P(("dp", "ep"), None, None),
        P(("dp", "ep"), None, None),
        P(("dp", "ep")),
    )
    return jax.shard_map(
        shards,
        mesh=mesh,
        in_specs=placed,
        out_specs=(P(("dp", "ep"), None), P(("dp", "ep"), None)),
        check_vma=False,
    )
```

```python
import math

import jax
import jax.numpy as jnp
from jax import lax
from jax.sharding import PartitionSpec as P


HEADS = 16
HEAD_DIM = 128
FRAME_TOK = 24

WEIGHT_MATE = (1, 0, 3, 2)
ROW_MATE = (3, 2, 1, 0)


def ring_swap(mate):
    return [(2 * ring + core, 2 * mate[ring] + core) for ring in range(4) for core in range(2)]


WEIGHT_SWAP = ring_swap(WEIGHT_MATE)
ROW_SWAP = ring_swap(ROW_MATE)
CORE_SWAP = [(place, place ^ 1) for place in range(8)]


def activate(pre):
    return jax.nn.gelu(pre, approximate=True).astype(jnp.bfloat16)


def expert_slots(expert_ids):
    flat_ids = expert_ids.reshape(-1)
    assigned = flat_ids.shape[0]
    row_ids = lax.broadcasted_iota(jnp.int32, (assigned, assigned), 0)
    col_ids = lax.broadcasted_iota(jnp.int32, (assigned, assigned), 1)
    same_expert = (flat_ids[:, None] == flat_ids[None, :]) & (col_ids < row_ids)
    return jnp.sum(same_expert.astype(jnp.int32), axis=1).reshape(expert_ids.shape)


def attend(queries, span_keys, span_values, cache_keys, cache_values, valid_count):
    token_count = queries.shape[0]
    cache_len = cache_keys.shape[0]
    key_rows = jnp.concatenate([cache_keys, span_keys], axis=0)
    value_rows = jnp.concatenate([cache_values, span_values], axis=0)
    query_heads = queries.reshape(token_count, HEADS, HEAD_DIM)
    key_heads = key_rows.reshape(-1, HEADS, HEAD_DIM)
    value_heads = value_rows.reshape(-1, HEADS, HEAD_DIM)
    scores = jnp.einsum(
        "thd,khd->htk", query_heads, key_heads, preferred_element_type=jnp.float32
    ) * (1.0 / math.sqrt(HEAD_DIM))
    position = lax.broadcasted_iota(jnp.int32, (key_rows.shape[0],), 0)
    usable = (position >= cache_len) | (position // FRAME_TOK < valid_count)
    scores = jnp.where(usable[None, None, :], scores, -1e30)
    row_max = jnp.max(scores, axis=2, keepdims=True)
    weights = jnp.exp(scores - row_max)
    weights = (weights / jnp.sum(weights, axis=2, keepdims=True)).astype(jnp.bfloat16)
    result = jnp.einsum("htk,khd->thd", weights, value_heads, preferred_element_type=jnp.float32)
    return result.astype(jnp.bfloat16).reshape(token_count, HEADS * HEAD_DIM)


def in_order(swapped, first, second):
    return [jnp.where(swapped, second, first), jnp.where(swapped, first, second)]


def pair_order(ring, core, blocks):
    own = jnp.concatenate(in_order(core == 1, blocks[0], blocks[1]), axis=1)
    mate = jnp.concatenate(in_order(core == 1, blocks[2], blocks[3]), axis=1)
    return jnp.concatenate(in_order(ring % 2 == 1, own, mate), axis=1)


def swap(block, pairs):
    return lax.ppermute(block, "dp", pairs)


def both_cores(block):
    mate = swap(block, WEIGHT_SWAP)
    return [block, swap(block, CORE_SWAP), mate, swap(mate, CORE_SWAP)]


def shards(
    hidden_in,
    expert_ids,
    route_logits,
    first_weight,
    second_weight,
    queries,
    span_keys,
    span_values,
    cache_keys,
    cache_values,
    valid_frames,
):
    tokens, model_width = hidden_in.shape
    experts = lax.axis_size("ep")
    place = lax.axis_index("dp")
    ring, core = place // 2, place % 2
    upper = ring // 2

    first_parts = both_cores(first_weight[0])
    second_parts = both_cores(second_weight[0])

    slots = expert_slots(expert_ids)
    places = expert_ids * 4 + upper * 2 + slots
    expert_cols = lax.broadcasted_iota(jnp.int32, route_logits.shape, 1)
    chosen = jnp.stack(
        [
            jnp.sum(
                jnp.where(expert_cols == expert_ids[:, column : column + 1], route_logits, 0.0),
                axis=1,
            )
            for column in range(2)
        ],
        axis=1,
    )
    gates = jax.nn.softmax(chosen, axis=1)
    notes = jnp.concatenate([places.astype(jnp.float32), gates], axis=1)
    both_notes = jnp.concatenate([notes, swap(notes, ROW_SWAP)], axis=0)
    both_places = both_notes[:, :2].astype(jnp.int32)
    both_gates = both_notes[:, 2:]
    both_hidden = jnp.concatenate([hidden_in, swap(hidden_in, ROW_SWAP)], axis=0)
    place_ids = lax.broadcasted_iota(jnp.int32, (2 * tokens, experts * 4), 1)
    picks = [both_places[:, column : column + 1] == place_ids for column in range(2)]
    chooser = (picks[0] | picks[1]).astype(jnp.bfloat16)

    dispatch = lax.dot_general(
        chooser, both_hidden, (((0,), (0,)), ((), ())), preferred_element_type=jnp.float32
    )
    dispatch = dispatch.astype(jnp.bfloat16).reshape(experts, 4, model_width)
    received = lax.all_to_all(dispatch, "ep", split_axis=0, concat_axis=0, tiled=True)
    expert_rows = received.reshape(experts * 4, model_width)

    act = pair_order(
        ring,
        core,
        [
            activate(jnp.dot(expert_rows, part, preferred_element_type=jnp.float32))
            for part in first_parts
        ],
    )
    other_act = swap(act, ROW_SWAP)
    all_act = jnp.concatenate(in_order(upper == 1, act, other_act), axis=1)

    outputs = jnp.concatenate(
        [
            jnp.dot(all_act, part, preferred_element_type=jnp.float32).astype(jnp.bfloat16)
            for part in second_parts
        ],
        axis=1,
    )
    returned = lax.all_to_all(
        outputs.reshape(experts, 4, -1), "ep", split_axis=0, concat_axis=0, tiled=True
    )
    flat_back = returned.reshape(experts * 4, -1)

    attended = attend(
        queries, span_keys, span_values, cache_keys[0], cache_values[0], valid_frames[0]
    )

    running = jnp.zeros((2 * tokens, flat_back.shape[1]), jnp.float32)
    for column in range(2):
        picked = jnp.dot(
            picks[column].astype(jnp.bfloat16), flat_back, preferred_element_type=jnp.float32
        )
        running = running + both_gates[:, column : column + 1] * picked
    mixed = running.astype(jnp.bfloat16)
    mixed = pair_order(ring, core, jnp.split(mixed, 4, axis=1))
    other_mixed = swap(mixed[tokens:], ROW_SWAP)
    mixed = jnp.concatenate(in_order(upper == 1, mixed[:tokens], other_mixed), axis=1)
    return (mixed, attended)


def solution(mesh):
    placed = (
        P(("dp", "ep"), None),
        P(("dp", "ep"), None),
        P(("dp", "ep"), None),
        P("ep", None, "dp"),
        P("ep", None, "dp"),
        P(("dp", "ep"), None),
        P(("dp", "ep"), None),
        P(("dp", "ep"), None),
        P(("dp", "ep"), None, None),
        P(("dp", "ep"), None, None),
        P(("dp", "ep")),
    )
    return jax.shard_map(
        shards,
        mesh=mesh,
        in_specs=placed,
        out_specs=(P(("dp", "ep"), None), P(("dp", "ep"), None)),
        check_vma=False,
    )
```

```python
import math

import jax
import jax.numpy as jnp
from jax import lax
from jax.experimental import pallas as pl
from jax.experimental.pallas import tpu as pltpu
from jax.sharding import PartitionSpec as P


HEADS = 16
HEAD_DIM = 128
FRAME_TOK = 24

CORE_FLIP, FIRST_FLIP, ROW_FLIP, SECOND_FLIP = 1, 2, 4, 6
ACT_BLOCK = 256


def activate(pre):
    return jax.nn.gelu(pre, approximate=True).astype(jnp.bfloat16)


def expert_slots(expert_ids):
    flat_ids = expert_ids.reshape(-1)
    assigned = flat_ids.shape[0]
    row_ids = lax.broadcasted_iota(jnp.int32, (assigned, assigned), 0)
    col_ids = lax.broadcasted_iota(jnp.int32, (assigned, assigned), 1)
    same_expert = (flat_ids[:, None] == flat_ids[None, :]) & (col_ids < row_ids)
    return jnp.sum(same_expert.astype(jnp.int32), axis=1).reshape(expert_ids.shape)


def attend(queries, span_keys, span_values, cache_keys, cache_values, valid_count):
    token_count = queries.shape[0]
    cache_len = cache_keys.shape[0]
    key_rows = jnp.concatenate([cache_keys, span_keys], axis=0)
    value_rows = jnp.concatenate([cache_values, span_values], axis=0)
    query_heads = queries.reshape(token_count, HEADS, HEAD_DIM)
    key_heads = key_rows.reshape(-1, HEADS, HEAD_DIM)
    value_heads = value_rows.reshape(-1, HEADS, HEAD_DIM)
    scores = jnp.einsum(
        "thd,khd->htk", query_heads, key_heads, preferred_element_type=jnp.float32
    ) * (1.0 / math.sqrt(HEAD_DIM))
    position = lax.broadcasted_iota(jnp.int32, (key_rows.shape[0],), 0)
    usable = (position >= cache_len) | (position // FRAME_TOK < valid_count)
    scores = jnp.where(usable[None, None, :], scores, -1e30)
    row_max = jnp.max(scores, axis=2, keepdims=True)
    weights = jnp.exp(scores - row_max)
    weights = (weights / jnp.sum(weights, axis=2, keepdims=True)).astype(jnp.bfloat16)
    result = jnp.einsum("htk,khd->thd", weights, value_heads, preferred_element_type=jnp.float32)
    return result.astype(jnp.bfloat16).reshape(token_count, HEADS * HEAD_DIM)


def swap(block, flip):
    return lax.ppermute(block, "dp", [(place, place ^ flip) for place in range(8)])


def four_parts(block, flip, pieces):
    mate = jnp.concatenate(
        [swap(piece, flip) for piece in jnp.split(block, pieces, axis=0)],
        axis=0,
    )
    return [block, swap(block, CORE_FLIP), mate, swap(mate, CORE_FLIP)]


def dispatch_kernel(choose_ref, own_ref, mate_ref, out_ref):
    choose = choose_ref[...]
    half = choose.shape[1] // 2
    rows = jnp.dot(choose[:, :half], own_ref[...], preferred_element_type=jnp.float32)
    rows += jnp.dot(choose[:, half:], mate_ref[...], preferred_element_type=jnp.float32)
    out_ref[...] = rows.astype(jnp.bfloat16).reshape(out_ref.shape)


def dispatch_rows(choose, own, mate, items):
    count, width = choose.shape[0], own.shape[1]
    tokens, step = own.shape[0], 1024
    return pl.pallas_call(
        dispatch_kernel,
        grid=(width // step,),
        in_specs=[pl.BlockSpec(choose.shape, lambda i: (0, 0))]
        + [pl.BlockSpec((tokens, step), lambda i: (0, i))] * 2,
        out_specs=pl.BlockSpec((items, count // items, step), lambda i: (0, 0, i)),
        out_shape=jax.ShapeDtypeStruct((items, count // items, width), jnp.bfloat16),
        name="dispatch_rows",
    )(choose, own, mate)


def first_kernel(place_ref, rows_ref, left_ref, right_ref, act_ref, sums):
    step = pl.program_id(0)

    @pl.when(step == 0)
    def _():
        sums[...] = jnp.zeros_like(sums)

    rows = rows_ref[...].reshape(sums.shape[0], -1)
    wide = jnp.concatenate([left_ref[...], right_ref[...]], axis=1)
    sums[...] += jnp.dot(rows, wide, preferred_element_type=jnp.float32)

    @pl.when(step == pl.num_programs(0) - 1)
    def _():
        odd = place_ref[0] % 2 == 1
        half = ACT_BLOCK // 2
        act = activate(sums[...])
        left, right = act[:, :half], act[:, half:]
        act_ref[:, :half] = jnp.where(odd, right, left)
        act_ref[:, half:] = jnp.where(odd, left, right)


def first_stage(place, rows, left, right):
    items, slots, depth = rows.shape
    count, wide, step = items * slots, left.shape[1], 1024
    return pl.pallas_call(
        first_kernel,
        grid_spec=pltpu.PrefetchScalarGridSpec(
            num_scalar_prefetch=1,
            grid=(depth // step,),
            in_specs=[pl.BlockSpec((items, slots, step), lambda i, p: (0, 0, i))]
            + [pl.BlockSpec((step, wide), lambda i, p: (i, 0))] * 2,
            out_specs=pl.BlockSpec((count, ACT_BLOCK), lambda i, p: (0, 0)),
            scratch_shapes=[pltpu.VMEM((count, ACT_BLOCK), jnp.float32)],
        ),
        out_shape=jax.ShapeDtypeStruct((count, ACT_BLOCK), jnp.bfloat16),
        name="first_stage",
    )(place, rows, left, right)


def near_kernel(place_ref, even_ref, odd_ref, *refs):
    part_refs, sums_ref = refs[:4], refs[4]
    step = pl.program_id(0)
    wide = part_refs[0].shape[1]
    act = jnp.where(step == 0, even_ref[...], odd_ref[...])

    @pl.when(step == 0)
    def _():
        for index, part_ref in enumerate(part_refs):
            sums_ref[:, index * wide : (index + 1) * wide] = jnp.dot(
                act, part_ref[...], preferred_element_type=jnp.float32
            )

    @pl.when(step > 0)
    def _():
        for index, part_ref in enumerate(part_refs):
            sums_ref[:, index * wide : (index + 1) * wide] += jnp.dot(
                act, part_ref[...], preferred_element_type=jnp.float32
            )


def far_kernel(place_ref, even_ref, odd_ref, *refs):
    part_refs, before_ref, out_ref, sums = refs[:4], refs[4], refs[5], refs[6]
    step = pl.program_id(0)
    wide = part_refs[0].shape[1]
    act = jnp.where(step == 0, even_ref[...], odd_ref[...])

    @pl.when(step == 0)
    def _():
        for index, part_ref in enumerate(part_refs):
            lanes = slice(index * wide, (index + 1) * wide)
            sums[:, lanes] = before_ref[:, lanes] + jnp.dot(
                act, part_ref[...], preferred_element_type=jnp.float32
            )

    @pl.when(step > 0)
    def _():
        for index, part_ref in enumerate(part_refs):
            lanes = slice(index * wide, (index + 1) * wide)
            total = sums[:, lanes] + jnp.dot(
                act, part_ref[...], preferred_element_type=jnp.float32
            )
            out_ref[:, :, lanes] = total.astype(jnp.bfloat16).reshape(out_ref.shape[:2] + (wide,))


def second_stage(place, acts, parts, before=None, items=None):
    count = acts[0].shape[0]
    wide = parts[0].shape[1]
    width = 4 * wide
    near = before is None
    first_block = 0 if near else 2
    whole = pl.BlockSpec((count, width), lambda i, p: (0, 0))
    in_specs = [pl.BlockSpec((count, ACT_BLOCK), lambda i, p: (0, 0))] * 2 + [
        pl.BlockSpec((ACT_BLOCK, wide), lambda i, p: ((p[0] // 2) ^ (i + first_block), 0))
    ] * 4
    if near:
        return pl.pallas_call(
            near_kernel,
            grid_spec=pltpu.PrefetchScalarGridSpec(
                num_scalar_prefetch=1, grid=(2,), in_specs=in_specs, out_specs=whole
            ),
            out_shape=jax.ShapeDtypeStruct((count, width), jnp.float32),
            name="second_near",
        )(place, *acts, *parts)
    shape = (items, count // items, width)
    return pl.pallas_call(
        far_kernel,
        grid_spec=pltpu.PrefetchScalarGridSpec(
            num_scalar_prefetch=1,
            grid=(2,),
            in_specs=in_specs + [whole],
            out_specs=pl.BlockSpec(shape, lambda i, p: (0, 0, 0)),
            scratch_shapes=[pltpu.VMEM((count, width), jnp.float32)],
        ),
        out_shape=jax.ShapeDtypeStruct(shape, jnp.bfloat16),
        name="second_far",
    )(place, *acts, *parts, before)


def shards(
    hidden_in,
    expert_ids,
    route_logits,
    first_weight,
    second_weight,
    queries,
    span_keys,
    span_values,
    cache_keys,
    cache_values,
    valid_frames,
):
    tokens, model_width = hidden_in.shape
    experts = lax.axis_size("ep")
    place = lax.axis_index("dp")
    place_list = place.reshape(1).astype(jnp.int32)

    first_parts = four_parts(first_weight[0], FIRST_FLIP, 1)
    second_parts = four_parts(second_weight[0], SECOND_FLIP, 1)

    tail = jnp.pad(expert_ids.astype(jnp.bfloat16), ((0, 0), (0, 126)))
    mate_rows = swap(jnp.concatenate([hidden_in, tail], axis=1), ROW_FLIP)
    ids_mate = mate_rows[:, model_width : model_width + 2].astype(jnp.int32)
    upper = place // 4
    places = jnp.concatenate(
        [
            expert_ids * 4 + 2 * upper + expert_slots(expert_ids),
            ids_mate * 4 + 2 * (1 - upper) + expert_slots(ids_mate),
        ],
        axis=0,
    )
    place_ids = lax.broadcasted_iota(jnp.int32, (2 * tokens, experts * 4), 1)
    picks = [places[:, column : column + 1] == place_ids for column in range(2)]
    place_rows = lax.broadcasted_iota(jnp.int32, (experts * 4, 2 * tokens), 0)
    choose = (places[:, 0][None, :] == place_rows) | (places[:, 1][None, :] == place_rows)

    dispatch = dispatch_rows(choose.astype(jnp.bfloat16), hidden_in, mate_rows, experts)
    received = lax.all_to_all(dispatch, "ep", split_axis=0, concat_axis=0, tiled=True)

    near, far = [], []
    for index in range(2):
        left, right = first_parts[2 * index : 2 * index + 2]
        act = first_stage(place_list, received, left, right)
        near.append(act)
        far.append(swap(act, ROW_FLIP))

    expert_cols = lax.broadcasted_iota(jnp.int32, route_logits.shape, 1)
    chosen = jnp.stack(
        [
            jnp.sum(
                jnp.where(expert_cols == expert_ids[:, column : column + 1], route_logits, 0.0),
                axis=1,
            )
            for column in range(2)
        ],
        axis=1,
    )
    gates = jax.nn.softmax(chosen, axis=1)
    both_gates = jnp.concatenate([gates, swap(gates, ROW_FLIP)], axis=0)

    sums = second_stage(place_list, near, second_parts)
    outputs = second_stage(place_list, far, second_parts, sums, experts)
    width = outputs.shape[2]
    returned = lax.all_to_all(outputs, "ep", split_axis=0, concat_axis=0, tiled=True)
    flat_back = returned.reshape(experts * 4, width)

    attended = attend(
        queries, span_keys, span_values, cache_keys[0], cache_values[0], valid_frames[0]
    )

    running = jnp.zeros((2 * tokens, width), jnp.float32)
    for column in range(2):
        picked = jnp.dot(
            picks[column].astype(jnp.bfloat16), flat_back, preferred_element_type=jnp.float32
        )
        running = running + both_gates[:, column : column + 1] * picked
    halves = running.astype(jnp.bfloat16)
    arrived = swap(halves[tokens:], ROW_FLIP)
    flips = (0, CORE_FLIP, SECOND_FLIP, SECOND_FLIP ^ CORE_FLIP)
    blocks = [None] * 8
    for half, flip in ((halves[:tokens], 0), (arrived, ROW_FLIP)):
        for index, block in enumerate(jnp.split(half, 4, axis=1)):
            blocks[flips[index] ^ flip] = block
    for bit in (1, 2, 4):
        turned = (place & bit) != 0
        blocks = [jnp.where(turned, blocks[index ^ bit], blocks[index]) for index in range(8)]
    mixed = jnp.concatenate(blocks, axis=1)
    return (mixed, attended)


def solution(mesh):
    placed = (
        P(("dp", "ep"), None),
        P(("dp", "ep"), None),
        P(("dp", "ep"), None),
        P("ep", None, "dp"),
        P("ep", None, "dp"),
        P(("dp", "ep"), None),
        P(("dp", "ep"), None),
        P(("dp", "ep"), None),
        P(("dp", "ep"), None, None),
        P(("dp", "ep"), None, None),
        P(("dp", "ep")),
    )
    return jax.shard_map(
        shards,
        mesh=mesh,
        in_specs=placed,
        out_specs=(P(("dp", "ep"), None), P(("dp", "ep"), None)),
        check_vma=False,
    )
```

```python
import math

import jax
import jax.numpy as jnp
from jax import lax
from jax.experimental import pallas as pl
from jax.experimental.pallas import tpu as pltpu
from jax.sharding import PartitionSpec as P


HEADS = 16
HEAD_DIM = 128
FRAME_TOK = 24

CORE_FLIP, FIRST_FLIP, ROW_FLIP, SECOND_FLIP = 1, 2, 4, 6
SIDE_FLIP = 8
ACT_BLOCK = 256


def activate(pre):
    return jax.nn.gelu(pre, approximate=True).astype(jnp.bfloat16)


def expert_slots(expert_ids):
    flat_ids = expert_ids.reshape(-1)
    assigned = flat_ids.shape[0]
    row_ids = lax.broadcasted_iota(jnp.int32, (assigned, assigned), 0)
    col_ids = lax.broadcasted_iota(jnp.int32, (assigned, assigned), 1)
    same_expert = (flat_ids[:, None] == flat_ids[None, :]) & (col_ids < row_ids)
    return jnp.sum(same_expert.astype(jnp.int32), axis=1).reshape(expert_ids.shape)


def attend(queries, span_keys, span_values, cache_keys, cache_values, valid_count):
    token_count = queries.shape[0]
    cache_len = cache_keys.shape[0]
    key_rows = jnp.concatenate([cache_keys, span_keys], axis=0)
    value_rows = jnp.concatenate([cache_values, span_values], axis=0)
    query_heads = queries.reshape(token_count, HEADS, HEAD_DIM)
    key_heads = key_rows.reshape(-1, HEADS, HEAD_DIM)
    value_heads = value_rows.reshape(-1, HEADS, HEAD_DIM)
    scores = jnp.einsum(
        "thd,khd->htk", query_heads, key_heads, preferred_element_type=jnp.float32
    ) * (1.0 / math.sqrt(HEAD_DIM))
    position = lax.broadcasted_iota(jnp.int32, (key_rows.shape[0],), 0)
    usable = (position >= cache_len) | (position // FRAME_TOK < valid_count)
    scores = jnp.where(usable[None, None, :], scores, -1e30)
    row_max = jnp.max(scores, axis=2, keepdims=True)
    weights = jnp.exp(scores - row_max)
    weights = (weights / jnp.sum(weights, axis=2, keepdims=True)).astype(jnp.bfloat16)
    result = jnp.einsum("htk,khd->thd", weights, value_heads, preferred_element_type=jnp.float32)
    return result.astype(jnp.bfloat16).reshape(token_count, HEADS * HEAD_DIM)


def swap(block, flip):
    return lax.ppermute(block, "dp", [(place, place ^ flip) for place in range(8)])


def swap_far(block, places, flip):
    return lax.ppermute(block, ("dp", "ep"), [(i, i ^ flip) for i in range(places)])


def four_parts(block, flip, pieces):
    mate = jnp.concatenate(
        [swap(piece, flip) for piece in jnp.split(block, pieces, axis=0)],
        axis=0,
    )
    return [block, swap(block, CORE_FLIP), mate, swap(mate, CORE_FLIP)]


def dispatch_kernel(choose_ref, *refs):
    token_refs, out_ref = refs[:-1], refs[-1]
    tokens = token_refs[0].shape[0]
    rows = None
    for index, token_ref in enumerate(token_refs):
        part = jnp.dot(
            choose_ref[:, index * tokens : (index + 1) * tokens],
            token_ref[...],
            preferred_element_type=jnp.float32,
        )
        rows = part if rows is None else rows + part
    out_ref[...] = rows.astype(jnp.bfloat16)


def dispatch_rows(choose, streams):
    tokens, width = streams[0].shape
    count, step = choose.shape[0], 1024
    return pl.pallas_call(
        dispatch_kernel,
        grid=(width // step,),
        in_specs=[pl.BlockSpec(choose.shape, lambda i: (0, 0))]
        + [pl.BlockSpec((tokens, step), lambda i: (0, i))] * len(streams),
        out_specs=pl.BlockSpec((count, step), lambda i: (0, i)),
        out_shape=jax.ShapeDtypeStruct((count, width), jnp.bfloat16),
        name="dispatch_rows",
    )(choose, *streams)


def first_kernel(place_ref, rows_ref, left_ref, right_ref, act_ref, sums):
    step = pl.program_id(0)

    @pl.when(step == 0)
    def _():
        sums[...] = jnp.zeros_like(sums)

    rows = rows_ref[...]
    wide = jnp.concatenate([left_ref[...], right_ref[...]], axis=1)
    sums[...] += jnp.dot(rows, wide, preferred_element_type=jnp.float32)

    @pl.when(step == pl.num_programs(0) - 1)
    def _():
        odd = place_ref[0] % 2 == 1
        half = ACT_BLOCK // 2
        act = activate(sums[...])
        left, right = act[:, :half], act[:, half:]
        act_ref[:, :half] = jnp.where(odd, right, left)
        act_ref[:, half:] = jnp.where(odd, left, right)


def first_stage(place, rows, left, right):
    count, depth = rows.shape
    wide, step = left.shape[1], 1024
    return pl.pallas_call(
        first_kernel,
        grid_spec=pltpu.PrefetchScalarGridSpec(
            num_scalar_prefetch=1,
            grid=(depth // step,),
            in_specs=[pl.BlockSpec((count, step), lambda i, p: (0, i))]
            + [pl.BlockSpec((step, wide), lambda i, p: (i, 0))] * 2,
            out_specs=pl.BlockSpec((count, ACT_BLOCK), lambda i, p: (0, 0)),
            scratch_shapes=[pltpu.VMEM((count, ACT_BLOCK), jnp.float32)],
        ),
        out_shape=jax.ShapeDtypeStruct((count, ACT_BLOCK), jnp.bfloat16),
        name="first_stage",
    )(place, rows, left, right)


def near_kernel(place_ref, even_ref, odd_ref, *refs):
    part_refs, sums_ref = refs[:4], refs[4]
    step = pl.program_id(0)
    wide = part_refs[0].shape[1]
    act = jnp.where(step == 0, even_ref[...], odd_ref[...])

    @pl.when(step == 0)
    def _():
        for index, part_ref in enumerate(part_refs):
            sums_ref[:, index * wide : (index + 1) * wide] = jnp.dot(
                act, part_ref[...], preferred_element_type=jnp.float32
            )

    @pl.when(step > 0)
    def _():
        for index, part_ref in enumerate(part_refs):
            sums_ref[:, index * wide : (index + 1) * wide] += jnp.dot(
                act, part_ref[...], preferred_element_type=jnp.float32
            )


def far_kernel(place_ref, even_ref, odd_ref, *refs):
    part_refs, before_ref, out_ref, sums = refs[:4], refs[4], refs[5], refs[6]
    step = pl.program_id(0)
    wide = part_refs[0].shape[1]
    act = jnp.where(step == 0, even_ref[...], odd_ref[...])

    @pl.when(step == 0)
    def _():
        for index, part_ref in enumerate(part_refs):
            lanes = slice(index * wide, (index + 1) * wide)
            sums[:, lanes] = before_ref[:, lanes] + jnp.dot(
                act, part_ref[...], preferred_element_type=jnp.float32
            )

    @pl.when(step > 0)
    def _():
        for index, part_ref in enumerate(part_refs):
            lanes = slice(index * wide, (index + 1) * wide)
            total = sums[:, lanes] + jnp.dot(
                act, part_ref[...], preferred_element_type=jnp.float32
            )
            outer, sides, inner, slots, _ = out_ref.shape
            total = total.reshape(outer, inner, sides * slots, wide).astype(jnp.bfloat16)
            for side in range(sides):
                out_ref[:, side, :, :, lanes] = total[:, :, side * slots : (side + 1) * slots, :]


def second_stage(place, acts, parts, before=None, form=None):
    count = acts[0].shape[0]
    wide = parts[0].shape[1]
    width = 4 * wide
    near = before is None
    first_block = 0 if near else 2
    whole = pl.BlockSpec((count, width), lambda i, p: (0, 0))
    in_specs = [pl.BlockSpec((count, ACT_BLOCK), lambda i, p: (0, 0))] * 2 + [
        pl.BlockSpec((ACT_BLOCK, wide), lambda i, p: ((p[0] // 2) ^ (i + first_block), 0))
    ] * 4
    if near:
        return pl.pallas_call(
            near_kernel,
            grid_spec=pltpu.PrefetchScalarGridSpec(
                num_scalar_prefetch=1, grid=(2,), in_specs=in_specs, out_specs=whole
            ),
            out_shape=jax.ShapeDtypeStruct((count, width), jnp.float32),
            name="second_near",
        )(place, *acts, *parts)
    shape = form + (width,)
    return pl.pallas_call(
        far_kernel,
        grid_spec=pltpu.PrefetchScalarGridSpec(
            num_scalar_prefetch=1,
            grid=(2,),
            in_specs=in_specs + [whole],
            out_specs=pl.BlockSpec(shape, lambda i, p: (0,) * len(shape)),
            scratch_shapes=[pltpu.VMEM((count, width), jnp.float32)],
        ),
        out_shape=jax.ShapeDtypeStruct(shape, jnp.bfloat16),
        name="second_far",
    )(place, *acts, *parts, before)


def shards(
    hidden_in,
    expert_ids,
    route_logits,
    first_weight,
    second_weight,
    queries,
    span_keys,
    span_values,
    cache_keys,
    cache_values,
    valid_frames,
):
    tokens, model_width = hidden_in.shape
    experts = lax.axis_size("ep")
    place = lax.axis_index("dp")
    place_list = place.reshape(1).astype(jnp.int32)

    first_parts = four_parts(first_weight[0], FIRST_FLIP, 1)
    second_parts = four_parts(second_weight[0], SECOND_FLIP, 1)

    tail = jnp.pad(expert_ids.astype(jnp.bfloat16), ((0, 0), (0, 126)))
    rows = jnp.concatenate([hidden_in, tail], axis=1)
    devices = lax.axis_size("dp") * experts
    row_flip = ROW_FLIP * experts
    mates = [swap_far(rows, devices, flip) for flip in (row_flip, SIDE_FLIP, row_flip ^ SIDE_FLIP)]
    all_ids = [expert_ids] + [
        mate[:, model_width : model_width + 2].astype(jnp.int32) for mate in mates
    ]
    all_slots = [expert_slots(ids) for ids in all_ids]
    upper = place // 4
    side = (lax.axis_index("ep") // SIDE_FLIP) % 2
    send_places = []
    for index, (ids, slots) in enumerate(zip(all_ids, all_slots)):
        source_side, stream = side ^ (index // 2), upper ^ (index % 2)
        column = (ids // (2 * SIDE_FLIP)) * SIDE_FLIP + ids % SIDE_FLIP
        sent = (ids // SIDE_FLIP) % 2 == side
        send_places.append(jnp.where(sent, column * 8 + source_side * 4 + stream * 2 + slots, -1))
    send_places = jnp.concatenate(send_places, axis=0)
    send_rows = lax.broadcasted_iota(jnp.int32, (experts * 4, 4 * tokens), 0)
    choose = (send_places[:, 0][None, :] == send_rows) | (send_places[:, 1][None, :] == send_rows)
    places = jnp.concatenate(
        [all_ids[0] * 4 + 2 * upper + all_slots[0], all_ids[1] * 4 + 2 * (1 - upper) + all_slots[1]],
        axis=0,
    )
    place_ids = lax.broadcasted_iota(jnp.int32, (2 * tokens, experts * 4), 1)
    picks = [places[:, column : column + 1] == place_ids for column in range(2)]

    dispatch = dispatch_rows(choose.astype(jnp.bfloat16), [hidden_in] + mates)
    sides = [[e for e in range(experts) if e // SIDE_FLIP % 2 == side] for side in range(2)]
    received = lax.all_to_all(
        dispatch.reshape(experts // 2, 8, model_width),
        "ep",
        split_axis=0,
        concat_axis=0,
        tiled=True,
        axis_index_groups=sides,
    ).reshape(experts * 4, model_width)

    near, far = [], []
    for index in range(2):
        left, right = first_parts[2 * index : 2 * index + 2]
        act = first_stage(place_list, received, left, right)
        near.append(act)
        far.append(swap(act, ROW_FLIP))

    expert_cols = lax.broadcasted_iota(jnp.int32, route_logits.shape, 1)
    chosen = jnp.stack(
        [
            jnp.sum(
                jnp.where(expert_cols == expert_ids[:, column : column + 1], route_logits, 0.0),
                axis=1,
            )
            for column in range(2)
        ],
        axis=1,
    )
    gates = jax.nn.softmax(chosen, axis=1)
    both_gates = jnp.concatenate([gates, swap(gates, ROW_FLIP)], axis=0)

    sums = second_stage(place_list, near, second_parts)
    form = (experts // (2 * SIDE_FLIP), 2, SIDE_FLIP, 4)
    outputs = second_stage(place_list, far, second_parts, sums, form)
    width = outputs.shape[-1]
    outputs = outputs.reshape(experts, 4, width)
    returned = lax.all_to_all(outputs, "ep", split_axis=0, concat_axis=0, tiled=True)
    flat_back = returned.reshape(experts * 4, width)

    attended = attend(
        queries, span_keys, span_values, cache_keys[0], cache_values[0], valid_frames[0]
    )

    running = jnp.zeros((2 * tokens, width), jnp.float32)
    for column in range(2):
        picked = jnp.dot(
            picks[column].astype(jnp.bfloat16), flat_back, preferred_element_type=jnp.float32
        )
        running = running + both_gates[:, column : column + 1] * picked
    halves = running.astype(jnp.bfloat16)
    arrived = swap(halves[tokens:], ROW_FLIP)
    flips = (0, CORE_FLIP, SECOND_FLIP, SECOND_FLIP ^ CORE_FLIP)
    blocks = [None] * 8
    for half, flip in ((halves[:tokens], 0), (arrived, ROW_FLIP)):
        for index, block in enumerate(jnp.split(half, 4, axis=1)):
            blocks[flips[index] ^ flip] = block
    for bit in (1, 2, 4):
        turned = (place & bit) != 0
        blocks = [jnp.where(turned, blocks[index ^ bit], blocks[index]) for index in range(8)]
    mixed = jnp.concatenate(blocks, axis=1)
    return (mixed, attended)


def solution(mesh):
    placed = (
        P(("dp", "ep"), None),
        P(("dp", "ep"), None),
        P(("dp", "ep"), None),
        P("ep", None, "dp"),
        P("ep", None, "dp"),
        P(("dp", "ep"), None),
        P(("dp", "ep"), None),
        P(("dp", "ep"), None),
        P(("dp", "ep"), None, None),
        P(("dp", "ep"), None, None),
        P(("dp", "ep")),
    )
    return jax.shard_map(
        shards,
        mesh=mesh,
        in_specs=placed,
        out_specs=(P(("dp", "ep"), None), P(("dp", "ep"), None)),
        check_vma=False,
    )
```

```python
import math

import jax
import jax.numpy as jnp
from jax import lax
from jax.experimental import pallas as pl
from jax.experimental.pallas import tpu as pltpu
from jax.sharding import PartitionSpec as P


HEADS = 16
HEAD_DIM = 128
FRAME_TOK = 24

CORE_FLIP, FIRST_FLIP, ROW_FLIP, SECOND_FLIP = 1, 2, 4, 6
ACT_BLOCK = 256


def activate(pre):
    return jax.nn.gelu(pre, approximate=True).astype(jnp.bfloat16)


def expert_slots(expert_ids):
    flat_ids = expert_ids.reshape(-1)
    assigned = flat_ids.shape[0]
    row_ids = lax.broadcasted_iota(jnp.int32, (assigned, assigned), 0)
    col_ids = lax.broadcasted_iota(jnp.int32, (assigned, assigned), 1)
    same_expert = (flat_ids[:, None] == flat_ids[None, :]) & (col_ids < row_ids)
    return jnp.sum(same_expert.astype(jnp.int32), axis=1).reshape(expert_ids.shape)


def attend(queries, span_keys, span_values, cache_keys, cache_values, valid_count):
    token_count = queries.shape[0]
    cache_len = cache_keys.shape[0]
    key_rows = jnp.concatenate([cache_keys, span_keys], axis=0)
    value_rows = jnp.concatenate([cache_values, span_values], axis=0)
    query_heads = queries.reshape(token_count, HEADS, HEAD_DIM)
    key_heads = key_rows.reshape(-1, HEADS, HEAD_DIM)
    value_heads = value_rows.reshape(-1, HEADS, HEAD_DIM)
    scores = jnp.einsum(
        "thd,khd->htk", query_heads, key_heads, preferred_element_type=jnp.float32
    ) * (1.0 / math.sqrt(HEAD_DIM))
    position = lax.broadcasted_iota(jnp.int32, (key_rows.shape[0],), 0)
    usable = (position >= cache_len) | (position // FRAME_TOK < valid_count)
    scores = jnp.where(usable[None, None, :], scores, -1e30)
    row_max = jnp.max(scores, axis=2, keepdims=True)
    weights = jnp.exp(scores - row_max)
    weights = (weights / jnp.sum(weights, axis=2, keepdims=True)).astype(jnp.bfloat16)
    result = jnp.einsum("htk,khd->thd", weights, value_heads, preferred_element_type=jnp.float32)
    return result.astype(jnp.bfloat16).reshape(token_count, HEADS * HEAD_DIM)


def swap(block, flip):
    return lax.ppermute(block, "dp", [(place, place ^ flip) for place in range(8)])


def four_parts(block, flip, pieces):
    mate = jnp.concatenate(
        [swap(piece, flip) for piece in jnp.split(block, pieces, axis=0)],
        axis=0,
    )
    return [block, swap(block, CORE_FLIP), mate, swap(mate, CORE_FLIP)]


def in_vmem(kernel, shape, dtype, place, *operands, to_hbm=False):
    operands = [pltpu.with_memory_space_constraint(operand, pltpu.VMEM) for operand in operands]
    specs = [pl.BlockSpec(memory_space=pltpu.VMEM)] * len(operands)
    if place is not None:
        operands, specs = [place] + operands, [pl.BlockSpec(memory_space=pltpu.SMEM)] + specs
    return pl.pallas_call(
        kernel,
        in_specs=specs,
        out_specs=pl.BlockSpec(memory_space=pltpu.VMEM),
        out_shape=jax.ShapeDtypeStruct(shape, dtype) if to_hbm else pltpu.VMEM(shape, dtype),
        compiler_params=pltpu.CompilerParams(vmem_limit_bytes=8 << 20),
    )(*operands)


def dispatch_kernel(choose_ref, *refs):
    token_refs, out_ref = refs[:-1], refs[-1]
    tokens, width = token_refs[0].shape[0], out_ref.shape[-1]
    step = 512
    for at in range(0, width, step):
        lanes = slice(at, at + step)
        rows = None
        for index, token_ref in enumerate(token_refs):
            part = jnp.dot(
                choose_ref[:, index * tokens : (index + 1) * tokens],
                token_ref[:, lanes],
                preferred_element_type=jnp.float32,
            )
            rows = part if rows is None else rows + part
        out_ref[..., lanes] = rows.astype(jnp.bfloat16).reshape(out_ref.shape[:-1] + (step,))


def first_kernel(place_ref, rows_ref, left_ref, right_ref, act_ref):
    depth, half, step = left_ref.shape[0], left_ref.shape[1], 1024
    total = None
    for at in range(0, depth, step):
        lanes = slice(at, at + step)
        rows = rows_ref[..., lanes].reshape(act_ref.shape[0], step)
        wide = jnp.concatenate([left_ref[lanes, :], right_ref[lanes, :]], axis=1)
        part = jnp.dot(rows, wide, preferred_element_type=jnp.float32)
        total = part if total is None else total + part
    act = activate(total)
    odd = place_ref[0] % 2 == 1
    left, right = act[:, :half], act[:, half:]
    act_ref[:, :half] = jnp.where(odd, right, left)
    act_ref[:, half:] = jnp.where(odd, left, right)


def second_dot(place_ref, even_ref, odd_ref, part_ref, first_block):
    ring = place_ref[0] // 2
    base = ((ring ^ first_block) // 2) * (2 * ACT_BLOCK)
    base = pl.multiple_of(base, 2 * ACT_BLOCK)
    turned = ring % 2 == 1
    even, odd = even_ref[...], odd_ref[...]
    act = jnp.concatenate([jnp.where(turned, odd, even), jnp.where(turned, even, odd)], axis=1)
    return jnp.dot(
        act, part_ref[pl.ds(base, 2 * ACT_BLOCK), :], preferred_element_type=jnp.float32
    )


def near_kernel(place_ref, even_ref, odd_ref, *refs):
    part_refs, sums_ref = refs[:4], refs[4]
    wide = part_refs[0].shape[1]
    for index, part_ref in enumerate(part_refs):
        lanes = slice(index * wide, (index + 1) * wide)
        sums_ref[:, lanes] = second_dot(place_ref, even_ref, odd_ref, part_ref, 0)


def far_kernel(place_ref, even_ref, odd_ref, *refs):
    part_refs, before_ref, out_ref = refs[:4], refs[4], refs[5]
    wide = part_refs[0].shape[1]
    for index, part_ref in enumerate(part_refs):
        lanes = slice(index * wide, (index + 1) * wide)
        total = before_ref[:, lanes] + second_dot(place_ref, even_ref, odd_ref, part_ref, 2)
        out_ref[..., lanes] = total.astype(jnp.bfloat16).reshape(out_ref.shape[:-1] + (wide,))


def shards(
    hidden_in,
    expert_ids,
    route_logits,
    first_weight,
    second_weight,
    queries,
    span_keys,
    span_values,
    cache_keys,
    cache_values,
    valid_frames,
):
    tokens, model_width = hidden_in.shape
    experts = lax.axis_size("ep")
    place = lax.axis_index("dp")
    place_list = place.reshape(1).astype(jnp.int32)

    first_parts = four_parts(first_weight[0], FIRST_FLIP, 1)
    second_parts = four_parts(second_weight[0], SECOND_FLIP, 1)

    tail = jnp.pad(expert_ids.astype(jnp.bfloat16), ((0, 0), (0, 126)))
    mate_rows = swap(jnp.concatenate([hidden_in, tail], axis=1), ROW_FLIP)
    ids_mate = mate_rows[:, model_width : model_width + 2].astype(jnp.int32)
    upper = place // 4
    places = jnp.concatenate(
        [
            expert_ids * 4 + 2 * upper + expert_slots(expert_ids),
            ids_mate * 4 + 2 * (1 - upper) + expert_slots(ids_mate),
        ],
        axis=0,
    )
    place_ids = lax.broadcasted_iota(jnp.int32, (2 * tokens, experts * 4), 1)
    picks = [places[:, column : column + 1] == place_ids for column in range(2)]
    place_rows = lax.broadcasted_iota(jnp.int32, (experts * 4, 2 * tokens), 0)
    choose = (places[:, 0][None, :] == place_rows) | (places[:, 1][None, :] == place_rows)

    dispatch = in_vmem(
        dispatch_kernel,
        (experts, 4, model_width),
        jnp.bfloat16,
        None,
        choose.astype(jnp.bfloat16),
        hidden_in,
        mate_rows,
        to_hbm=True,
    )
    received = lax.all_to_all(dispatch, "ep", split_axis=0, concat_axis=0, tiled=True)

    near, far = [], []
    for index in range(2):
        left, right = first_parts[2 * index : 2 * index + 2]
        act = in_vmem(
            first_kernel, (experts * 4, ACT_BLOCK), jnp.bfloat16, place_list, received, left, right
        )
        near.append(act)
        far.append(swap(act, ROW_FLIP))

    expert_cols = lax.broadcasted_iota(jnp.int32, route_logits.shape, 1)
    chosen = jnp.stack(
        [
            jnp.sum(
                jnp.where(expert_cols == expert_ids[:, column : column + 1], route_logits, 0.0),
                axis=1,
            )
            for column in range(2)
        ],
        axis=1,
    )
    gates = jax.nn.softmax(chosen, axis=1)
    both_gates = jnp.concatenate([gates, swap(gates, ROW_FLIP)], axis=0)

    width = 4 * second_parts[0].shape[1]
    sums = in_vmem(near_kernel, (experts * 4, width), jnp.float32, place_list, *near, *second_parts)
    outputs = in_vmem(
        far_kernel,
        (experts, 4) + (width,),
        jnp.bfloat16,
        place_list,
        *far,
        *second_parts,
        sums,
        to_hbm=True,
    )
    returned = lax.all_to_all(outputs, "ep", split_axis=0, concat_axis=0, tiled=True)
    flat_back = returned.reshape(experts * 4, width)

    attended = attend(
        queries, span_keys, span_values, cache_keys[0], cache_values[0], valid_frames[0]
    )

    running = jnp.zeros((2 * tokens, width), jnp.float32)
    for column in range(2):
        picked = jnp.dot(
            picks[column].astype(jnp.bfloat16), flat_back, preferred_element_type=jnp.float32
        )
        running = running + both_gates[:, column : column + 1] * picked
    halves = running.astype(jnp.bfloat16)
    arrived = swap(halves[tokens:], ROW_FLIP)
    flips = (0, CORE_FLIP, SECOND_FLIP, SECOND_FLIP ^ CORE_FLIP)
    blocks = [None] * 8
    for half, flip in ((halves[:tokens], 0), (arrived, ROW_FLIP)):
        for index, block in enumerate(jnp.split(half, 4, axis=1)):
            blocks[flips[index] ^ flip] = block
    for bit in (1, 2, 4):
        turned = (place & bit) != 0
        blocks = [jnp.where(turned, blocks[index ^ bit], blocks[index]) for index in range(8)]
    mixed = jnp.concatenate(blocks, axis=1)
    return (mixed, attended)


def solution(mesh):
    placed = (
        P(("dp", "ep"), None),
        P(("dp", "ep"), None),
        P(("dp", "ep"), None),
        P("ep", None, "dp"),
        P("ep", None, "dp"),
        P(("dp", "ep"), None),
        P(("dp", "ep"), None),
        P(("dp", "ep"), None),
        P(("dp", "ep"), None, None),
        P(("dp", "ep"), None, None),
        P(("dp", "ep")),
    )
    return jax.shard_map(
        shards,
        mesh=mesh,
        in_specs=placed,
        out_specs=(P(("dp", "ep"), None), P(("dp", "ep"), None)),
        check_vma=False,
    )
```

```python
import math

import jax
import jax.numpy as jnp
from jax import lax
from jax.experimental import pallas as pl
from jax.experimental.pallas import tpu as pltpu
from jax.sharding import PartitionSpec as P


HEADS = 16
HEAD_DIM = 128
FRAME_TOK = 24

CORE_FLIP, FIRST_FLIP, ROW_FLIP, SECOND_FLIP = 1, 2, 4, 6
ACT_BLOCK = 256


def activate(pre):
    return jax.nn.gelu(pre, approximate=True).astype(jnp.bfloat16)


def expert_slots(expert_ids):
    flat_ids = expert_ids.reshape(-1)
    assigned = flat_ids.shape[0]
    row_ids = lax.broadcasted_iota(jnp.int32, (assigned, assigned), 0)
    col_ids = lax.broadcasted_iota(jnp.int32, (assigned, assigned), 1)
    same_expert = (flat_ids[:, None] == flat_ids[None, :]) & (col_ids < row_ids)
    return jnp.sum(same_expert.astype(jnp.int32), axis=1).reshape(expert_ids.shape)


def attend(queries, span_keys, span_values, cache_keys, cache_values, valid_count):
    token_count = queries.shape[0]
    cache_len = cache_keys.shape[0]
    key_rows = jnp.concatenate([cache_keys, span_keys], axis=0)
    value_rows = jnp.concatenate([cache_values, span_values], axis=0)
    query_heads = queries.reshape(token_count, HEADS, HEAD_DIM)
    key_heads = key_rows.reshape(-1, HEADS, HEAD_DIM)
    value_heads = value_rows.reshape(-1, HEADS, HEAD_DIM)
    scores = jnp.einsum(
        "thd,khd->htk", query_heads, key_heads, preferred_element_type=jnp.float32
    ) * (1.0 / math.sqrt(HEAD_DIM))
    position = lax.broadcasted_iota(jnp.int32, (key_rows.shape[0],), 0)
    usable = (position >= cache_len) | (position // FRAME_TOK < valid_count)
    scores = jnp.where(usable[None, None, :], scores, -1e30)
    row_max = jnp.max(scores, axis=2, keepdims=True)
    weights = jnp.exp(scores - row_max)
    weights = (weights / jnp.sum(weights, axis=2, keepdims=True)).astype(jnp.bfloat16)
    result = jnp.einsum("htk,khd->thd", weights, value_heads, preferred_element_type=jnp.float32)
    return result.astype(jnp.bfloat16).reshape(token_count, HEADS * HEAD_DIM)


def swap(block, flip):
    return lax.ppermute(block, "dp", [(place, place ^ flip) for place in range(8)])


def four_parts(block, flip, pieces):
    mate = jnp.concatenate(
        [swap(piece, flip) for piece in jnp.split(block, pieces, axis=0)],
        axis=0,
    )
    return [block, swap(block, CORE_FLIP), mate, swap(mate, CORE_FLIP)]


def in_vmem(kernel, shape, dtype, place, *operands, to_hbm=False):
    operands = [pltpu.with_memory_space_constraint(operand, pltpu.VMEM) for operand in operands]
    specs = [pl.BlockSpec(memory_space=pltpu.VMEM)] * len(operands)
    if place is not None:
        operands, specs = [place] + operands, [pl.BlockSpec(memory_space=pltpu.SMEM)] + specs
    return pl.pallas_call(
        kernel,
        in_specs=specs,
        out_specs=pl.BlockSpec(memory_space=pltpu.VMEM),
        out_shape=jax.ShapeDtypeStruct(shape, dtype) if to_hbm else pltpu.VMEM(shape, dtype),
        compiler_params=pltpu.CompilerParams(vmem_limit_bytes=8 << 20),
    )(*operands)


def dispatch_kernel(choose_ref, *refs):
    token_refs, out_ref = refs[:-1], refs[-1]
    tokens, width = token_refs[0].shape[0], out_ref.shape[-1]
    step = 512
    for at in range(0, width, step):
        lanes = slice(at, at + step)
        rows = None
        for index, token_ref in enumerate(token_refs):
            part = jnp.dot(
                choose_ref[:, index * tokens : (index + 1) * tokens],
                token_ref[:, lanes],
                preferred_element_type=jnp.float32,
            )
            rows = part if rows is None else rows + part
        out_ref[..., lanes] = rows.astype(jnp.bfloat16).reshape(out_ref.shape[:-1] + (step,))


def first_kernel(place_ref, rows_ref, left_ref, right_ref, act_ref):
    depth, half, step = left_ref.shape[0], left_ref.shape[1], 1024
    total = None
    for at in range(0, depth, step):
        lanes = slice(at, at + step)
        rows = rows_ref[..., lanes].reshape(act_ref.shape[0], step)
        wide = jnp.concatenate([left_ref[lanes, :], right_ref[lanes, :]], axis=1)
        part = jnp.dot(rows, wide, preferred_element_type=jnp.float32)
        total = part if total is None else total + part
    act = activate(total)
    odd = place_ref[0] % 2 == 1
    left, right = act[:, :half], act[:, half:]
    act_ref[:, :half] = jnp.where(odd, right, left)
    act_ref[:, half:] = jnp.where(odd, left, right)


def ring_dot(place_ref, act_ref, part_ref, flip):
    base = pl.multiple_of(((place_ref[0] // 2) ^ flip) * ACT_BLOCK, ACT_BLOCK)
    return jnp.dot(
        act_ref[...], part_ref[pl.ds(base, ACT_BLOCK), :], preferred_element_type=jnp.float32
    )


def near_kernel(place_ref, own_ref, mate_ref, far_ref, *refs):
    part_refs, sums_ref = refs[:4], refs[4]
    wide = part_refs[0].shape[1]
    for index, part_ref in enumerate(part_refs):
        total = ring_dot(place_ref, own_ref, part_ref, 0)
        total += ring_dot(place_ref, mate_ref, part_ref, 1)
        total += ring_dot(place_ref, far_ref, part_ref, 2)
        sums_ref[:, index * wide : (index + 1) * wide] = total


def far_kernel(place_ref, far_ref, *refs):
    part_refs, before_ref, out_ref = refs[:4], refs[4], refs[5]
    wide = part_refs[0].shape[1]
    for index, part_ref in enumerate(part_refs):
        lanes = slice(index * wide, (index + 1) * wide)
        total = before_ref[:, lanes] + ring_dot(place_ref, far_ref, part_ref, 3)
        out_ref[..., lanes] = total.astype(jnp.bfloat16).reshape(out_ref.shape[:-1] + (wide,))


def shards(
    hidden_in,
    expert_ids,
    route_logits,
    first_weight,
    second_weight,
    queries,
    span_keys,
    span_values,
    cache_keys,
    cache_values,
    valid_frames,
):
    tokens, model_width = hidden_in.shape
    experts = lax.axis_size("ep")
    place = lax.axis_index("dp")
    place_list = place.reshape(1).astype(jnp.int32)

    first_parts = four_parts(first_weight[0], FIRST_FLIP, 1)
    second_parts = four_parts(second_weight[0], SECOND_FLIP, 1)

    tail = jnp.pad(expert_ids.astype(jnp.bfloat16), ((0, 0), (0, 126)))
    mate_rows = swap(jnp.concatenate([hidden_in, tail], axis=1), ROW_FLIP)
    ids_mate = mate_rows[:, model_width : model_width + 2].astype(jnp.int32)
    upper = place // 4
    places = jnp.concatenate(
        [
            expert_ids * 4 + 2 * upper + expert_slots(expert_ids),
            ids_mate * 4 + 2 * (1 - upper) + expert_slots(ids_mate),
        ],
        axis=0,
    )
    place_ids = lax.broadcasted_iota(jnp.int32, (2 * tokens, experts * 4), 1)
    picks = [places[:, column : column + 1] == place_ids for column in range(2)]
    place_rows = lax.broadcasted_iota(jnp.int32, (experts * 4, 2 * tokens), 0)
    choose = (places[:, 0][None, :] == place_rows) | (places[:, 1][None, :] == place_rows)

    dispatch = in_vmem(
        dispatch_kernel,
        (experts, 4, model_width),
        jnp.bfloat16,
        None,
        choose.astype(jnp.bfloat16),
        hidden_in,
        mate_rows,
        to_hbm=True,
    )
    received = lax.all_to_all(dispatch, "ep", split_axis=0, concat_axis=0, tiled=True)

    near, far = [], []
    for index in range(2):
        left, right = first_parts[2 * index : 2 * index + 2]
        act = in_vmem(
            first_kernel, (experts * 4, ACT_BLOCK), jnp.bfloat16, place_list, received, left, right
        )
        near.append(act)
        far.append(swap(act, ROW_FLIP))

    expert_cols = lax.broadcasted_iota(jnp.int32, route_logits.shape, 1)
    chosen = jnp.stack(
        [
            jnp.sum(
                jnp.where(expert_cols == expert_ids[:, column : column + 1], route_logits, 0.0),
                axis=1,
            )
            for column in range(2)
        ],
        axis=1,
    )
    gates = jax.nn.softmax(chosen, axis=1)
    both_gates = jnp.concatenate([gates, swap(gates, ROW_FLIP)], axis=0)

    width = 4 * second_parts[0].shape[1]
    sums = in_vmem(
        near_kernel, (experts * 4, width), jnp.float32, place_list, *near, far[0], *second_parts
    )
    outputs = in_vmem(
        far_kernel,
        (experts, 4) + (width,),
        jnp.bfloat16,
        place_list,
        far[1],
        *second_parts,
        sums,
        to_hbm=True,
    )
    returned = lax.all_to_all(outputs, "ep", split_axis=0, concat_axis=0, tiled=True)
    flat_back = returned.reshape(experts * 4, width)

    attended = attend(
        queries, span_keys, span_values, cache_keys[0], cache_values[0], valid_frames[0]
    )

    running = jnp.zeros((2 * tokens, width), jnp.float32)
    for column in range(2):
        picked = jnp.dot(
            picks[column].astype(jnp.bfloat16), flat_back, preferred_element_type=jnp.float32
        )
        running = running + both_gates[:, column : column + 1] * picked
    halves = running.astype(jnp.bfloat16)
    arrived = swap(halves[tokens:], ROW_FLIP)
    flips = (0, CORE_FLIP, SECOND_FLIP, SECOND_FLIP ^ CORE_FLIP)
    blocks = [None] * 8
    for half, flip in ((halves[:tokens], 0), (arrived, ROW_FLIP)):
        for index, block in enumerate(jnp.split(half, 4, axis=1)):
            blocks[flips[index] ^ flip] = block
    for bit in (1, 2, 4):
        turned = (place & bit) != 0
        blocks = [jnp.where(turned, blocks[index ^ bit], blocks[index]) for index in range(8)]
    mixed = jnp.concatenate(blocks, axis=1)
    return (mixed, attended)


def solution(mesh):
    placed = (
        P(("dp", "ep"), None),
        P(("dp", "ep"), None),
        P(("dp", "ep"), None),
        P("ep", None, "dp"),
        P("ep", None, "dp"),
        P(("dp", "ep"), None),
        P(("dp", "ep"), None),
        P(("dp", "ep"), None),
        P(("dp", "ep"), None, None),
        P(("dp", "ep"), None, None),
        P(("dp", "ep")),
    )
    return jax.shard_map(
        shards,
        mesh=mesh,
        in_specs=placed,
        out_specs=(P(("dp", "ep"), None), P(("dp", "ep"), None)),
        check_vma=False,
    )
```

```python
import math

import jax
import jax.numpy as jnp
from jax import lax
from jax.experimental import pallas as pl
from jax.experimental.pallas import tpu as pltpu
from jax.sharding import PartitionSpec as P


HEADS = 16
HEAD_DIM = 128
FRAME_TOK = 24

CORE_FLIP, FIRST_FLIP, ROW_FLIP, SECOND_FLIP = 1, 2, 4, 6
ACT_BLOCK = 256


def activate(pre):
    return jax.nn.gelu(pre, approximate=True).astype(jnp.bfloat16)


def expert_slots(expert_ids):
    flat_ids = expert_ids.reshape(-1)
    assigned = flat_ids.shape[0]
    row_ids = lax.broadcasted_iota(jnp.int32, (assigned, assigned), 0)
    col_ids = lax.broadcasted_iota(jnp.int32, (assigned, assigned), 1)
    same_expert = (flat_ids[:, None] == flat_ids[None, :]) & (col_ids < row_ids)
    return jnp.sum(same_expert.astype(jnp.int32), axis=1).reshape(expert_ids.shape)


def attend(queries, span_keys, span_values, cache_keys, cache_values, valid_count):
    token_count = queries.shape[0]
    cache_len = cache_keys.shape[0]
    key_rows = jnp.concatenate([cache_keys, span_keys], axis=0)
    value_rows = jnp.concatenate([cache_values, span_values], axis=0)
    query_heads = queries.reshape(token_count, HEADS, HEAD_DIM)
    key_heads = key_rows.reshape(-1, HEADS, HEAD_DIM)
    value_heads = value_rows.reshape(-1, HEADS, HEAD_DIM)
    scores = jnp.einsum(
        "thd,khd->htk", query_heads, key_heads, preferred_element_type=jnp.float32
    ) * (1.0 / math.sqrt(HEAD_DIM))
    position = lax.broadcasted_iota(jnp.int32, (key_rows.shape[0],), 0)
    usable = (position >= cache_len) | (position // FRAME_TOK < valid_count)
    scores = jnp.where(usable[None, None, :], scores, -1e30)
    row_max = jnp.max(scores, axis=2, keepdims=True)
    weights = jnp.exp(scores - row_max)
    weights = (weights / jnp.sum(weights, axis=2, keepdims=True)).astype(jnp.bfloat16)
    result = jnp.einsum("htk,khd->thd", weights, value_heads, preferred_element_type=jnp.float32)
    return result.astype(jnp.bfloat16).reshape(token_count, HEADS * HEAD_DIM)


def swap(block, flip):
    return lax.ppermute(block, "dp", [(place, place ^ flip) for place in range(8)])


def four_parts(block, flip, pieces):
    mate = jnp.concatenate(
        [swap(piece, flip) for piece in jnp.split(block, pieces, axis=0)],
        axis=0,
    )
    return [block, swap(block, CORE_FLIP), mate, swap(mate, CORE_FLIP)]


def in_vmem(kernel, shape, dtype, place, *operands, to_hbm=False):
    operands = [pltpu.with_memory_space_constraint(operand, pltpu.VMEM) for operand in operands]
    specs = [pl.BlockSpec(memory_space=pltpu.VMEM)] * len(operands)
    if place is not None:
        operands, specs = [place] + operands, [pl.BlockSpec(memory_space=pltpu.SMEM)] + specs
    return pl.pallas_call(
        kernel,
        in_specs=specs,
        out_specs=pl.BlockSpec(memory_space=pltpu.VMEM),
        out_shape=jax.ShapeDtypeStruct(shape, dtype) if to_hbm else pltpu.VMEM(shape, dtype),
        compiler_params=pltpu.CompilerParams(vmem_limit_bytes=8 << 20),
    )(*operands)


def dispatch_kernel(choose_ref, *refs):
    token_refs, out_ref = refs[:-1], refs[-1]
    tokens, width = token_refs[0].shape[0], out_ref.shape[-1]
    step = 512
    for at in range(0, width, step):
        lanes = slice(at, at + step)
        rows = None
        for index, token_ref in enumerate(token_refs):
            part = jnp.dot(
                choose_ref[:, index * tokens : (index + 1) * tokens],
                token_ref[:, lanes],
                preferred_element_type=jnp.float32,
            )
            rows = part if rows is None else rows + part
        out_ref[..., lanes] = rows.astype(jnp.bfloat16).reshape(out_ref.shape[:-1] + (step,))


def first_kernel(place_ref, rows_ref, left_ref, right_ref, act_ref):
    depth, half, step = left_ref.shape[0], left_ref.shape[1], 1024
    total = None
    for at in range(0, depth, step):
        lanes = slice(at, at + step)
        rows = rows_ref[..., lanes].reshape(act_ref.shape[0], step)
        wide = jnp.concatenate([left_ref[lanes, :], right_ref[lanes, :]], axis=1)
        part = jnp.dot(rows, wide, preferred_element_type=jnp.float32)
        total = part if total is None else total + part
    act = activate(total)
    odd = place_ref[0] % 2 == 1
    left, right = act[:, :half], act[:, half:]
    act_ref[:, :half] = jnp.where(odd, right, left)
    act_ref[:, half:] = jnp.where(odd, left, right)


def second_dot(place_ref, even_ref, odd_ref, part_ref, first_block):
    ring = place_ref[0] // 2
    base = ((ring ^ first_block) // 2) * (2 * ACT_BLOCK)
    base = pl.multiple_of(base, 2 * ACT_BLOCK)
    turned = ring % 2 == 1
    even, odd = even_ref[...], odd_ref[...]
    act = jnp.concatenate([jnp.where(turned, odd, even), jnp.where(turned, even, odd)], axis=1)
    return jnp.dot(
        act, part_ref[pl.ds(base, 2 * ACT_BLOCK), :], preferred_element_type=jnp.float32
    )


def near_kernel(place_ref, even_ref, odd_ref, *refs):
    part_refs, sums_ref = refs[:4], refs[4]
    wide = part_refs[0].shape[1]
    for index, part_ref in enumerate(part_refs):
        lanes = slice(index * wide, (index + 1) * wide)
        sums_ref[:, lanes] = second_dot(place_ref, even_ref, odd_ref, part_ref, 0)


def far_kernel(place_ref, even_ref, odd_ref, *refs):
    part_refs, before_ref, out_ref = refs[:4], refs[4], refs[5]
    wide = part_refs[0].shape[1]
    for index, part_ref in enumerate(part_refs):
        lanes = slice(index * wide, (index + 1) * wide)
        total = before_ref[:, lanes] + second_dot(place_ref, even_ref, odd_ref, part_ref, 2)
        out_ref[..., lanes] = total.astype(jnp.bfloat16).reshape(out_ref.shape[:-1] + (wide,))


def combine_kernel(first_ref, second_ref, gates_ref, rows_ref, out_ref):
    width, step = out_ref.shape[1], 512
    for at in range(0, width, step):
        lanes = slice(at, at + step)
        rows = rows_ref[..., lanes].reshape(first_ref.shape[1], step)
        mixed = gates_ref[:, :1] * jnp.dot(
            first_ref[...], rows, preferred_element_type=jnp.float32
        )
        mixed += gates_ref[:, 1:] * jnp.dot(
            second_ref[...], rows, preferred_element_type=jnp.float32
        )
        out_ref[:, lanes] = mixed.astype(jnp.bfloat16)


def shards(
    hidden_in,
    expert_ids,
    route_logits,
    first_weight,
    second_weight,
    queries,
    span_keys,
    span_values,
    cache_keys,
    cache_values,
    valid_frames,
):
    tokens, model_width = hidden_in.shape
    experts = lax.axis_size("ep")
    place = lax.axis_index("dp")
    place_list = place.reshape(1).astype(jnp.int32)

    first_parts = four_parts(first_weight[0], FIRST_FLIP, 1)
    second_parts = four_parts(second_weight[0], SECOND_FLIP, 1)

    tail = jnp.pad(expert_ids.astype(jnp.bfloat16), ((0, 0), (0, 126)))
    mate_rows = swap(jnp.concatenate([hidden_in, tail], axis=1), ROW_FLIP)
    ids_mate = mate_rows[:, model_width : model_width + 2].astype(jnp.int32)
    upper = place // 4
    places = jnp.concatenate(
        [
            expert_ids * 4 + 2 * upper + expert_slots(expert_ids),
            ids_mate * 4 + 2 * (1 - upper) + expert_slots(ids_mate),
        ],
        axis=0,
    )
    place_ids = lax.broadcasted_iota(jnp.int32, (2 * tokens, experts * 4), 1)
    picks = [places[:, column : column + 1] == place_ids for column in range(2)]
    place_rows = lax.broadcasted_iota(jnp.int32, (experts * 4, 2 * tokens), 0)
    choose = (places[:, 0][None, :] == place_rows) | (places[:, 1][None, :] == place_rows)

    dispatch = in_vmem(
        dispatch_kernel,
        (experts, 4, model_width),
        jnp.bfloat16,
        None,
        choose.astype(jnp.bfloat16),
        hidden_in,
        mate_rows,
        to_hbm=True,
    )
    received = lax.all_to_all(dispatch, "ep", split_axis=0, concat_axis=0, tiled=True)

    near, far = [], []
    for index in range(2):
        left, right = first_parts[2 * index : 2 * index + 2]
        act = in_vmem(
            first_kernel, (experts * 4, ACT_BLOCK), jnp.bfloat16, place_list, received, left, right
        )
        near.append(act)
        far.append(swap(act, ROW_FLIP))

    expert_cols = lax.broadcasted_iota(jnp.int32, route_logits.shape, 1)
    chosen = jnp.stack(
        [
            jnp.sum(
                jnp.where(expert_cols == expert_ids[:, column : column + 1], route_logits, 0.0),
                axis=1,
            )
            for column in range(2)
        ],
        axis=1,
    )
    gates = jax.nn.softmax(chosen, axis=1)
    both_gates = jnp.concatenate([gates, swap(gates, ROW_FLIP)], axis=0)

    width = 4 * second_parts[0].shape[1]
    sums = in_vmem(near_kernel, (experts * 4, width), jnp.float32, place_list, *near, *second_parts)
    outputs = in_vmem(
        far_kernel,
        (experts, 4) + (width,),
        jnp.bfloat16,
        place_list,
        *far,
        *second_parts,
        sums,
        to_hbm=True,
    )
    returned = lax.all_to_all(outputs, "ep", split_axis=0, concat_axis=0, tiled=True)

    attended = attend(
        queries, span_keys, span_values, cache_keys[0], cache_values[0], valid_frames[0]
    )

    halves = []
    for at in (tokens, 0):
        picked = [pick[at : at + tokens].astype(jnp.bfloat16) for pick in picks]
        halves.append(
            in_vmem(
                combine_kernel,
                (tokens, width),
                jnp.bfloat16,
                None,
                *picked,
                both_gates[at : at + tokens],
                returned,
            )
        )
    arrived = swap(halves[0], ROW_FLIP)
    flips = (0, CORE_FLIP, SECOND_FLIP, SECOND_FLIP ^ CORE_FLIP)
    blocks = [None] * 8
    for half, flip in ((halves[1], 0), (arrived, ROW_FLIP)):
        for index, block in enumerate(jnp.split(half, 4, axis=1)):
            blocks[flips[index] ^ flip] = block
    for bit in (1, 2, 4):
        turned = (place & bit) != 0
        blocks = [jnp.where(turned, blocks[index ^ bit], blocks[index]) for index in range(8)]
    mixed = jnp.concatenate(blocks, axis=1)
    return (mixed, attended)


def solution(mesh):
    placed = (
        P(("dp", "ep"), None),
        P(("dp", "ep"), None),
        P(("dp", "ep"), None),
        P("ep", None, "dp"),
        P("ep", None, "dp"),
        P(("dp", "ep"), None),
        P(("dp", "ep"), None),
        P(("dp", "ep"), None),
        P(("dp", "ep"), None, None),
        P(("dp", "ep"), None, None),
        P(("dp", "ep")),
    )
    return jax.shard_map(
        shards,
        mesh=mesh,
        in_specs=placed,
        out_specs=(P(("dp", "ep"), None), P(("dp", "ep"), None)),
        check_vma=False,
    )
```
